32 devices in a mesh: gx: 2 (over x), gy: 4 (over y, core), gz: 4 (over z).
Axes of the slice: x: 2, y: 2, z: 4, core: 2. Of those that a mesh axis runs over, the one named last changes fastest.
Arguments:
- state: float32 [5, 12, 96, 1536], P(None, 'gx', 'gy', 'gz'), as said below
- register: float32 [5, 12, 96, 1536], P(None, 'gx', 'gy', 'gz'), may hold values from -0.25 to 0.25
Outputs:
- new_state: float32 [5, 12, 96, 1536], P(None, 'gx', 'gy', 'gz')
- new_register: float32 [5, 12, 96, 1536], P(None, 'gx', 'gy', 'gz')
The draws below stay inside these ranges and needn't reach their ends.
Inputs may be any that keep to these rules, and one draw needn't show every extreme that they name: Density is between 0.5 and 2.5, and the pressure computed from the state is positive.
All inputs are finite; a program needn't handle non-finite values.
Results may differ from the reference program's by a relative error of at most 0.0003.
Values sent between devices are 32-bit elements; how exact they have to be, the bound alone decides.
A program may use at most 128 MiB of HBM per device.

```python
import math
import jax
import jax.numpy as jnp
import numpy as np
from jax import lax

NVAR = 5
NXN = 12
NYN = 96
NZN = 1536


def smooth_field(key, grid, amplitude):
    xpos = lax.broadcasted_iota(jnp.float32, grid, 0) / grid[0]
    ypos = lax.broadcasted_iota(jnp.float32, grid, 1) / grid[1]
    zpos = lax.broadcasted_iota(jnp.float32, grid, 2) / grid[2]
    waves = jax.random.randint(jax.random.fold_in(key, 1), (4, 3), 1, 4).astype(jnp.float32)
    phases = jax.random.uniform(jax.random.fold_in(key, 2), (4,), jnp.float32, 0.0, 6.283185307179586)
    total = jnp.zeros(grid, jnp.float32)
    for mode in range(4):
        angle = 6.283185307179586 * (waves[mode, 0] * xpos + waves[mode, 1] * ypos + waves[mode, 2] * zpos) + phases[mode]
        total = total + amplitude * jnp.sin(angle)
    return total


def draw_state(key, part):
    key_rho = jax.random.fold_in(key, 11)
    key_vel = jax.random.fold_in(key, 12)
    key_press = jax.random.fold_in(key, 13)
    grid = (NXN, NYN, NZN)
    xpos = lax.broadcasted_iota(jnp.float32, grid, 0) / NXN
    amp = 1.0 + 2.0 * xpos
    noise = 0.015 * jnp.clip(jax.random.normal(jax.random.fold_in(key_vel, 5), (3,) + grid, jnp.float32), -3.0, 3.0)
    rho_noise = 0.03 * jnp.clip(jax.random.normal(jax.random.fold_in(key_rho, 5), grid, jnp.float32), -3.0, 3.0)
    press_noise = 0.03 * jnp.clip(jax.random.normal(jax.random.fold_in(key_press, 5), grid, jnp.float32), -3.0, 3.0)
    density = 1.0 + smooth_field(key_rho, grid, 0.08) + rho_noise
    press = 1.0 + smooth_field(key_press, grid, 0.08) + press_noise
    vel = jnp.stack([amp * smooth_field(jax.random.fold_in(key_vel, c), grid, 0.1) for c in range(3)]) + noise
    energy = press / 0.4 + 0.5 * density * jnp.sum(vel * vel, axis=0)
    return jnp.concatenate([density[None], density[None] * vel, energy[None]], axis=0).astype(jnp.float32)


def block_scale(rng, extent, pieces, smallest, high):
    loudness = 1.0
    for axis_at, blocks in pieces:
        heights = jax.random.uniform(jax.random.fold_in(jax.random.fold_in(rng, 6), axis_at), (blocks,), jnp.float32, smallest / len(pieces), high / len(pieces))
        loudness = loudness * jnp.repeat(jnp.exp(heights), extent[axis_at] // blocks).reshape((-1,) + (1,) * (len(extent) - 1 - axis_at))
    return loudness


def centred(stream_key, shape, deviation, limit, cuts=(), dtype=jnp.bfloat16):
    result = deviation * jax.random.normal(stream_key, shape, jnp.float32)
    if cuts:
        result = result * block_scale(stream_key, shape, cuts, -0.22, 0.18)
    return jnp.clip(result, -limit, limit).astype(dtype)


def setup_inputs(seed: int = 0) -> dict:
    splits = jax.random.split(jax.random.key(seed), 3)
    state = draw_state(jax.random.fold_in(splits[2], 71), 0)
    register = centred(splits[1], (NVAR, NXN, NYN, NZN), 0.05, 0.25, ((1, 2), (2, 4), (3, 4)), jnp.float32)
    return dict(state=state, register=register)


GAMMA = 1.4
GM1 = 0.4
ELEM_WIDTH = 0.05
COURANT = 0.5
INV_W = 15.0
COEFFS = ((-567301805773.0 / 1357537059087.0, 5161836677717.0 / 13612068292357.0), (-2404267990393.0 / 2016746695238.0, 1720146321549.0 / 2090206949498.0))
FORMS = ('ij,vejyz->veiyz', 'ij,vxejz->vxeiz', 'ij,vxyej->vxyei')

def gll_derivative():
    seven = math.sqrt(7.0)
    inner = math.sqrt(1.0 / 3.0 - 2.0 * seven / 21.0)
    outer = math.sqrt(1.0 / 3.0 + 2.0 * seven / 21.0)
    points = np.array([-1.0, -outer, -inner, inner, outer, 1.0])
    count = len(points)
    weights = np.array([np.prod([points[i] - points[j] for j in range(count) if j != i]) for i in range(count)])
    table = np.zeros((count, count))
    for i in range(count):
        for j in range(count):
            if i != j:
                table[i, j] = weights[i] / weights[j] / (points[i] - points[j])
        table[i, i] = -np.sum(table[i])
    return table

def pressure(u):
    mom_sq = u[1] * u[1] + u[2] * u[2] + u[3] * u[3]
    return (GM1 * (u[4] - 0.5 * mom_sq / u[0]), mom_sq)

def euler_flux(u, d):
    press, mom_sq = pressure(u)
    vel = u[1 + d] / u[0]
    parts = [u[1 + d], u[1] * vel, u[2] * vel, u[3] * vel, (u[4] + press) * vel]
    parts[1 + d] = parts[1 + d] + press
    speed = jnp.abs(vel) + jnp.sqrt(GAMMA * press / u[0])
    return (jnp.stack(parts), speed)

def direction_term(ext, d, diff):
    axis = 1 + d
    nodes = diff.shape[0]
    full = ext.shape[axis]
    length = full - 2
    elems = length // nodes
    inner = lax.slice_in_dim(ext, 1, full - 1, axis=axis)
    flux_in, unused = euler_flux(inner, d)
    shape = flux_in.shape
    blocked = flux_in.reshape(shape[:axis] + (elems, nodes) + shape[axis + 1:])
    deriv = jnp.einsum(FORMS[d], diff, blocked, precision=lax.Precision.HIGHEST).reshape(shape)
    lower_side = lax.slice_in_dim(ext, 0, length + 1, nodes, axis)
    upper_side = lax.slice_in_dim(ext, 1, length + 2, nodes, axis)
    flux_low, speed_low = euler_flux(lower_side, d)
    flux_up, speed_up = euler_flux(upper_side, d)
    lam = jnp.maximum(speed_low, speed_up)
    fstar = 0.5 * (flux_low + flux_up) - 0.5 * lam[None] * (upper_side - lower_side)
    first = lax.slice_in_dim(flux_in, 0, length, nodes, axis)
    last = lax.slice_in_dim(flux_in, nodes - 1, length, nodes, axis)
    lower = -(first - lax.slice_in_dim(fstar, 0, elems, axis=axis)) * INV_W
    upper = (last - lax.slice_in_dim(fstar, 1, elems + 1, axis=axis)) * INV_W
    bshape = shape[:axis] + (elems, 1) + shape[axis + 1:]
    zeros = jnp.zeros(shape[:axis] + (elems, nodes - 2) + shape[axis + 1:], jnp.float32)
    corr = jnp.concatenate([lower.reshape(bshape), zeros, upper.reshape(bshape)], axis=axis + 1).reshape(shape)
    return 2.0 / ELEM_WIDTH * (corr - deriv)

def max_speed(u):
    press, mom_sq = pressure(u)
    return jnp.max(jnp.sqrt(mom_sq) / u[0] + jnp.sqrt(GAMMA * press / u[0]))

def residual_of(u, diff):
    total = jnp.zeros_like(u)
    for d in range(3):
        pads = [(0, 0)] * 4
        pads[1 + d] = (1, 1)
        ext = jnp.pad(u, pads, mode='wrap')
        total = total + direction_term(ext, d, diff)
    return total

def reference(state, register):
    diff = jnp.asarray(gll_derivative(), jnp.float32)
    step = COURANT * ELEM_WIDTH / (11.0 * max_speed(state))
    current = state
    section_reg = register
    for coef_a, coef_b in COEFFS:
        section_reg = coef_a * section_reg + step * residual_of(current, diff)
        current = current + coef_b * section_reg
    return (current, section_reg)
```

```python
import functools
import math

import jax
import jax.numpy as jnp
import numpy as np
from jax import lax
from jax.experimental import pallas as pl
from jax.experimental.pallas import tpu as pltpu
from jax.sharding import PartitionSpec as P

GAMMA = 1.4
GM1 = 0.4
ELEM_WIDTH = 0.05
COURANT = 0.5
INV_W = 15.0
SCALE = 2.0 / ELEM_WIDTH
HALF = 0.5 * INV_W * SCALE
COEFFS = (
    (-567301805773.0 / 1357537059087.0, 5161836677717.0 / 13612068292357.0),
    (-2404267990393.0 / 2016746695238.0, 1720146321549.0 / 2090206949498.0),
)
AXES = ("gx", "gy", "gz")
NV = 5
SUB = 8
LANE = 128
MESH = pl.DeviceIdType.MESH


def gll_derivative():
    seven = math.sqrt(7.0)
    inner = math.sqrt(1.0 / 3.0 - 2.0 * seven / 21.0)
    outer = math.sqrt(1.0 / 3.0 + 2.0 * seven / 21.0)
    points = np.array([-1.0, -outer, -inner, inner, outer, 1.0])
    count = len(points)
    weights = np.array(
        [np.prod([points[i] - points[j] for j in range(count) if j != i]) for i in range(count)]
    )
    table = np.zeros((count, count))
    for i in range(count):
        for j in range(count):
            if i != j:
                table[i, j] = weights[i] / weights[j] / (points[i] - points[j])
        table[i, i] = -np.sum(table[i])
    return table


DMAT = gll_derivative()
NODES = DMAT.shape[0]


def operator(length):
    op = np.kron(np.eye(length // NODES), -SCALE * DMAT)
    for j in range(NODES, length, NODES):
        i = j - 1
        op[j, j] -= HALF
        op[j, i] += HALF
        op[i, j] -= HALF
        op[i, i] += HALF
    op[np.abs(op) < 1e-9] = 0.0
    return op


def split(table):
    high = np.asarray(table, np.float32).astype(jnp.bfloat16)
    low = (np.asarray(table, np.float32) - high.astype(np.float32)).astype(jnp.bfloat16)
    return np.stack([high, low])


def windows(length):
    op = operator(length).T
    count = length // LANE - 1
    out = np.zeros((count, 2 * LANE, 2 * LANE))
    for w in range(count):
        lo = 0 if w == 0 else LANE // 2
        hi = 2 * LANE if w == count - 1 else LANE + LANE // 2
        base = w * LANE
        out[w, :, lo:hi] = op[base : base + 2 * LANE, base + lo : base + hi]
    return out


def primitives(u):
    inv = 1.0 / u[0]
    mom_sq = u[1] * u[1] + u[2] * u[2] + u[3] * u[3]
    press = GM1 * (u[4] - 0.5 * mom_sq * inv)
    sound = jnp.sqrt(GAMMA * press * inv)
    return inv, mom_sq, press, sound


def flux_of(u, d, inv, press):
    vel = u[1 + d] * inv
    parts = [u[1 + d], u[1] * vel, u[2] * vel, u[3] * vel, (u[4] + press) * vel]
    parts[1 + d] = parts[1 + d] + press
    return parts, vel


def face_terms(low, up, d):
    inv_l, _, press_l, sound_l = primitives(low)
    inv_u, _, press_u, sound_u = primitives(up)
    flux_l, vel_l = flux_of(low, d, inv_l, press_l)
    flux_u, vel_u = flux_of(up, d, inv_u, press_u)
    lam = jnp.maximum(jnp.abs(vel_l) + sound_l, jnp.abs(vel_u) + sound_u)
    first, last = [], []
    for v in range(NV):
        central = HALF * (flux_u[v] - flux_l[v])
        jump = (HALF * lam) * (up[v] - low[v])
        first.append(-central - jump)
        last.append(jump - central)
    return first, last


def kernel(
    dims, sizes,
    state_ref, reg_ref, ly_ref, wz_ref, out_ref, reg_out_ref,
    u1_ref, acc_ref, fx_ref, fy_ref, fz_ref, sy_ref, sz_ref, step_ref,
    xh_ref, yp_ref, yh_ref, zp_ref, zh_ref, mcur_ref, mx_ref,
    xs_sem, xr_sem, ys_sem, yr_sem, zs_sem, zr_sem, ms_sem, mr_sem,
):
    nx, ny, nz = dims
    rows = nx * ny
    tiles = ny // SUB
    me = [lax.axis_index(a) for a in AXES]

    def peer(axis, offset):
        n = sizes[axis]
        return {AXES[axis]: lax.rem(me[axis] + (offset % n), n)}

    barrier = pltpu.get_barrier_semaphore()
    greeted = 0
    for axis in range(3):
        for off in range(1, sizes[axis]):
            pl.semaphore_signal(barrier, inc=1, device_id=peer(axis, off), device_id_type=MESH)
            greeted += 1
    pl.semaphore_wait(barrier, greeted)

    def remote(src, dst, ssem, rsem, axis, off):
        return pltpu.make_async_remote_copy(
            src_ref=src, dst_ref=dst, send_sem=ssem, recv_sem=rsem,
            device_id=peer(axis, off), device_id_type=MESH,
        )

    def x_copy(u_ref, sec, side, t):
        base = (rows - ny if side == 0 else 0) + t * SUB
        return remote(
            u_ref.at[:, pl.ds(base, SUB), :], xh_ref.at[sec, side, :, pl.ds(t * SUB, SUB), :],
            xs_sem.at[sec, side, t], xr_sem.at[sec, side, t], 0, 1 if side == 0 else -1,
        )

    def y_copy(sec, side):
        return remote(
            yp_ref.at[sec, 1 - side], yh_ref.at[sec, side],
            ys_sem.at[sec, side], yr_sem.at[sec, side], 1, 1 if side == 0 else -1,
        )

    def z_copy(sec, side):
        return remote(
            zp_ref.at[sec, 1 - side], zh_ref.at[sec, side],
            zs_sem.at[sec, side], zr_sem.at[sec, side], 2, 1 if side == 0 else -1,
        )

    def m_copy(axis, off):
        return remote(
            mcur_ref.at[axis], mx_ref.at[axis, off],
            ms_sem.at[axis, off], mr_sem.at[axis, off], axis, off,
        )

    lane_ids = lax.broadcasted_iota(jnp.int32, (ny, LANE), 1)

    def pack(u_ref, sec):
        for v in range(NV):
            for x in range(nx):
                a = x * ny
                yp_ref[sec, 0, v, x : x + 1, :] = u_ref[v, a : a + 1, :]
                yp_ref[sec, 1, v, x : x + 1, :] = u_ref[v, a + ny - 1 : a + ny, :]

        def one(v, carry):
            first = jnp.ones((ny, LANE), jnp.float32)
            last = first
            for x in range(nx):
                r = slice(x * ny, x * ny + ny)
                first = jnp.where(lane_ids == x, u_ref[v, r, 0:LANE][:, 0:1], first)
                last = jnp.where(lane_ids == x, u_ref[v, r, nz - LANE : nz][:, LANE - 1 : LANE], last)
            zp_ref[sec, 0, v] = first
            zp_ref[sec, 1, v] = last
            return carry

        lax.fori_loop(0, NV, one, 0)

    def pointwise(u_ref, want_max):
        def one(t, top):
            r = pl.ds(pl.multiple_of(t * SUB, SUB), SUB)
            u = [u_ref[v, r, :] for v in range(NV)]
            inv, mom_sq, press, sound = primitives(u)
            for d, f_ref in enumerate((fx_ref, fy_ref, fz_ref)):
                parts, vel = flux_of(u, d, inv, press)
                for v in range(NV):
                    f_ref[v, r, :] = parts[v]
                if d == 1:
                    sy_ref[r, :] = jnp.abs(vel) + sound
                if d == 2:
                    sz_ref[r, :] = jnp.abs(vel) + sound
            if want_max:
                speed = jnp.sqrt(mom_sq) * inv + sound
                for b in range(nz // LANE):
                    top = jnp.maximum(top, speed[:, b * LANE : (b + 1) * LANE])
            return top

        return lax.fori_loop(0, rows // SUB, one, jnp.zeros((SUB, LANE), jnp.float32))

    def halves(x):
        high = x.astype(jnp.bfloat16)
        return high, (x - high.astype(jnp.float32)).astype(jnp.bfloat16)

    def dot(a, b):
        return jnp.dot(a, b, preferred_element_type=jnp.float32)

    def products(v, carry):
        high, low = halves(fy_ref[v])
        acc_ref[v] = dot(ly_ref[0], high) + dot(ly_ref[0], low) + dot(ly_ref[1], high)
        high, low = halves(fz_ref[v])
        for w in range(nz // LANE - 1):
            c = slice(w * LANE, (w + 2) * LANE)
            acc_ref[v, :, c] += (
                dot(high[:, c], wz_ref[0, w]) + dot(low[:, c], wz_ref[0, w]) + dot(high[:, c], wz_ref[1, w])
            )
        return carry

    op_x = operator(nx)

    def along_x(t, carry):
        v = lax.div(t, tiles)
        base = lax.rem(t, tiles) * SUB
        where = [pl.ds(pl.multiple_of(base + i * ny, SUB), SUB) for i in range(nx)]
        f = [fx_ref[v, r, :] for r in where]
        for i in range(nx):
            total = acc_ref[v, where[i], :]
            for j in range(nx):
                if op_x[i, j] != 0.0:
                    total = total + float(op_x[i, j]) * f[j]
            acc_ref[v, where[i], :] = total
        return carry

    row_in = lax.broadcasted_iota(jnp.int32, (ny, nz), 0)
    lane_in = lax.broadcasted_iota(jnp.int32, (ny, nz), 1)

    def dissipate(u_ref):
        def one(x, carry):
            r = pl.ds(pl.multiple_of(x * ny, SUB), ny)
            s = sy_ref[r, :]
            mask = (lax.rem(row_in, NODES) == 0) & (row_in > 0)
            lam_y = jnp.where(mask, HALF * jnp.maximum(s, pltpu.roll(s, 1, 0)), 0.0)
            s = sz_ref[r, :]
            mask = (lax.rem(lane_in, NODES) == 0) & (lane_in > 0)
            lam_z = jnp.where(mask, HALF * jnp.maximum(s, pltpu.roll(s, 1, 1)), 0.0)
            for v in range(NV):
                u = u_ref[v, r, :]
                wy = lam_y * (u - pltpu.roll(u, 1, 0))
                wz = lam_z * (u - pltpu.roll(u, 1, 1))
                acc_ref[v, r, :] += (pltpu.roll(wy, ny - 1, 0) - wy) + (pltpu.roll(wz, nz - 1, 1) - wz)
            return carry

        lax.fori_loop(0, nx, one, 0)
        for e in range(NODES, nx, NODES):
            lo, up = (e - 1) * ny, e * ny
            for t in range(tiles):
                ra = slice(lo + t * SUB, lo + t * SUB + SUB)
                rb = slice(up + t * SUB, up + t * SUB + SUB)
                a = [u_ref[v, ra, :] for v in range(NV)]
                b = [u_ref[v, rb, :] for v in range(NV)]
                ia, _, _, ca = primitives(a)
                ib, _, _, cb = primitives(b)
                lam = HALF * jnp.maximum(jnp.abs(a[1] * ia) + ca, jnp.abs(b[1] * ib) + cb)
                for v in range(NV):
                    jump = lam * (b[v] - a[v])
                    acc_ref[v, rb, :] -= jump
                    acc_ref[v, ra, :] += jump

    def volume(u_ref):
        lax.fori_loop(0, NV, products, 0)
        lax.fori_loop(0, NV * tiles, along_x, 0)
        dissipate(u_ref)

    def edges_y(sec):
        for side in range(2):
            y_copy(sec, side).wait_recv()
            own = [yp_ref[sec, side, v] for v in range(NV)]
            other = [yh_ref[sec, side, v] for v in range(NV)]
            corr = face_terms(other, own, 1)[0] if side == 0 else face_terms(own, other, 1)[1]
            for v in range(NV):
                for x in range(nx):
                    a = x * ny + (0 if side == 0 else ny - 1)
                    acc_ref[v, a : a + 1, :] += corr[v][x : x + 1, :]

    def edges_z(sec):
        for side in range(2):
            z_copy(sec, side).wait_recv()
            own = [zp_ref[sec, side, v] for v in range(NV)]
            other = [zh_ref[sec, side, v] for v in range(NV)]
            corr = face_terms(other, own, 2)[0] if side == 0 else face_terms(own, other, 2)[1]
            at = 0 if side == 0 else LANE - 1
            c = slice(0, LANE) if side == 0 else slice(nz - LANE, nz)
            for v in range(NV):
                for x in range(nx):
                    r = slice(x * ny, x * ny + ny)
                    acc_ref[v, r, c] += jnp.where(lane_ids == at, corr[v][:, x : x + 1], 0.0)

    def advance(sec, r, corr=None):
        coef_a, coef_b = COEFFS[sec]
        src, old = (state_ref, reg_ref) if sec == 0 else (u1_ref, reg_out_ref)
        dst = u1_ref if sec == 0 else out_ref
        step = step_ref[...]
        for v in range(NV):
            res = acc_ref[v, r, :]
            if corr is not None:
                res = res + corr[v]
            k = coef_a * old[v, r, :] + step * res
            reg_out_ref[v, r, :] = k
            dst[v, r, :] = src[v, r, :] + coef_b * k

    def advance_inner(sec):
        def one(t, carry):
            advance(sec, pl.ds(pl.multiple_of(t * SUB, SUB), SUB))
            return carry

        lax.fori_loop(tiles, (nx - 1) * tiles, one, 0)

    def advance_outer(u_ref, sec, side, t):
        x_copy(u_ref, sec, side, t).wait_recv()
        base = (0 if side == 0 else rows - ny) + t * SUB
        r = slice(base, base + SUB)
        own = [u_ref[v, r, :] for v in range(NV)]
        other = [xh_ref[sec, side, v, t * SUB : (t + 1) * SUB, :] for v in range(NV)]
        corr = face_terms(other, own, 0)[0] if side == 0 else face_terms(own, other, 0)[1]
        advance(sec, r, corr)

    def reduce_max(axis, top):
        for off in range(1, sizes[axis]):
            m_copy(axis, off).wait_recv()
            top = jnp.maximum(top, mx_ref[axis, off])
        return top

    def send_max(axis):
        for off in range(1, sizes[axis]):
            m_copy(axis, off).start()

    order = [(t, side) for t in range(tiles) for side in range(2)]
    for t, side in order:
        x_copy(state_ref, 0, side, t).start()
    top = pointwise(state_ref, True)
    mcur_ref[2] = top
    pack(state_ref, 0)
    send_max(2)
    for side in range(2):
        y_copy(0, side).start()
        z_copy(0, side).start()
    lax.fori_loop(0, NV, products, 0)
    top = reduce_max(2, top)
    mcur_ref[1] = top
    lax.fori_loop(0, NV * tiles, along_x, 0)
    send_max(1)
    dissipate(state_ref)
    top = reduce_max(1, top)
    mcur_ref[0] = top
    edges_y(0)
    send_max(0)
    edges_z(0)
    top = reduce_max(0, top)
    top = jnp.max(jnp.max(top, axis=0, keepdims=True), axis=1, keepdims=True)
    step_ref[...] = jnp.broadcast_to(COURANT * ELEM_WIDTH / (11.0 * top), (SUB, nz))
    for t, side in order:
        advance_outer(state_ref, 0, side, t)
        x_copy(u1_ref, 1, 1 - side, t).start()
    advance_inner(0)
    pack(u1_ref, 1)
    pointwise(u1_ref, False)
    for side in range(2):
        y_copy(1, side).start()
        z_copy(1, side).start()
    volume(u1_ref)
    edges_y(1)
    edges_z(1)
    advance_inner(1)
    for t, side in order:
        advance_outer(u1_ref, 1, 1 - side, t)
    for axis in range(3):
        for off in range(1, sizes[axis]):
            m_copy(axis, off).wait_send()
    for sec in range(2):
        for side in range(2):
            y_copy(sec, side).wait_send()
            z_copy(sec, side).wait_send()
            for t in range(tiles):
                x_copy(state_ref if sec == 0 else u1_ref, sec, side, t).wait_send()


def shards(sizes, state, register):
    nx, ny, nz = state.shape[1:]
    rows = nx * ny
    tiles = ny // SUB
    most = max(sizes)
    f32 = jnp.float32
    flat = (NV, rows, nz)
    ly = jnp.asarray(split(np.kron(np.eye(nx), operator(ny))))
    wz = jnp.asarray(split(windows(nz)))
    vmem = pl.BlockSpec(memory_space=pltpu.VMEM)
    dma = pltpu.SemaphoreType.DMA
    new_state, new_reg = pl.pallas_call(
        functools.partial(kernel, (nx, ny, nz), sizes),
        out_shape=[jax.ShapeDtypeStruct(flat, f32)] * 2,
        in_specs=[vmem] * 4,
        out_specs=[vmem] * 2,
        scratch_shapes=[
            pltpu.VMEM(flat, f32), pltpu.VMEM(flat, f32),
            pltpu.VMEM(flat, f32), pltpu.VMEM(flat, f32), pltpu.VMEM(flat, f32),
            pltpu.VMEM((rows, nz), f32), pltpu.VMEM((rows, nz), f32),
            pltpu.VMEM((SUB, nz), f32),
            pltpu.VMEM((2, 2, NV, ny, nz), f32),
            pltpu.VMEM((2, 2, NV, nx, nz), f32), pltpu.VMEM((2, 2, NV, nx, nz), f32),
            pltpu.VMEM((2, 2, NV, ny, LANE), f32), pltpu.VMEM((2, 2, NV, ny, LANE), f32),
            pltpu.VMEM((3, SUB, LANE), f32), pltpu.VMEM((3, most, SUB, LANE), f32),
            dma((2, 2, tiles)), dma((2, 2, tiles)), dma((2, 2)), dma((2, 2)),
            dma((2, 2)), dma((2, 2)), dma((3, most)), dma((3, most)),
        ],
        compiler_params=pltpu.CompilerParams(
            collective_id=0, has_side_effects=True, vmem_limit_bytes=48 * 1024 * 1024
        ),
        name="dg_step",
    )(state.reshape(flat), register.reshape(flat), ly, wz)
    return new_state.reshape(state.shape), new_reg.reshape(state.shape)


def solution(mesh):
    sizes = tuple(mesh.shape[a] for a in AXES)
    spec = P(None, "gx", "gy", "gz")
    return jax.shard_map(
        functools.partial(shards, sizes),
        mesh=mesh,
        in_specs=(spec, spec),
        out_specs=(spec, spec),
        check_vma=False,
    )
```

```python
import functools
import math

import jax
import jax.numpy as jnp
import numpy as np
from jax import lax
from jax.experimental import pallas as pl
from jax.experimental.pallas import tpu as pltpu
from jax.sharding import PartitionSpec as P

GAMMA = 1.4
GM1 = 0.4
ELEM_WIDTH = 0.05
COURANT = 0.5
INV_W = 15.0
SCALE = 2.0 / ELEM_WIDTH
HALF = 0.5 * INV_W * SCALE
COEFFS = (
    (-567301805773.0 / 1357537059087.0, 5161836677717.0 / 13612068292357.0),
    (-2404267990393.0 / 2016746695238.0, 1720146321549.0 / 2090206949498.0),
)
AXES = ("gx", "gy", "gz")
NV = 5
SUB = 8
LANE = 128
GRANT = 60 * 1024 * 1024
MESH = pl.DeviceIdType.MESH


def gll_derivative():
    seven = math.sqrt(7.0)
    inner = math.sqrt(1.0 / 3.0 - 2.0 * seven / 21.0)
    outer = math.sqrt(1.0 / 3.0 + 2.0 * seven / 21.0)
    points = np.array([-1.0, -outer, -inner, inner, outer, 1.0])
    count = len(points)
    weights = np.array(
        [np.prod([points[i] - points[j] for j in range(count) if j != i]) for i in range(count)]
    )
    table = np.zeros((count, count))
    for i in range(count):
        for j in range(count):
            if i != j:
                table[i, j] = weights[i] / weights[j] / (points[i] - points[j])
        table[i, i] = -np.sum(table[i])
    return table


DMAT = gll_derivative()
NODES = DMAT.shape[0]


def operator(length):
    op = np.kron(np.eye(length // NODES), -SCALE * DMAT)
    for j in range(NODES, length, NODES):
        i = j - 1
        op[j, j] -= HALF
        op[j, i] += HALF
        op[i, j] -= HALF
        op[i, i] += HALF
    op[np.abs(op) < 1e-9] = 0.0
    return op


def split(table):
    high = np.asarray(table, np.float32).astype(jnp.bfloat16)
    low = (np.asarray(table, np.float32) - high.astype(np.float32)).astype(jnp.bfloat16)
    return np.stack([high, low])


def windows(length):
    op = operator(length).T
    count = length // LANE - 1
    out = np.zeros((count, 2 * LANE, 2 * LANE))
    for w in range(count):
        lo = 0 if w == 0 else LANE // 2
        hi = 2 * LANE if w == count - 1 else LANE + LANE // 2
        base = w * LANE
        out[w, :, lo:hi] = op[base : base + 2 * LANE, base + lo : base + hi]
    return out


def primitives(u):
    inv = 1.0 / u[0]
    mom_sq = u[1] * u[1] + u[2] * u[2] + u[3] * u[3]
    press = GM1 * (u[4] - 0.5 * mom_sq * inv)
    sound = jnp.sqrt(GAMMA * press * inv)
    return inv, mom_sq, press, sound


def flux_of(u, d, inv, press):
    vel = u[1 + d] * inv
    parts = [u[1 + d], u[1] * vel, u[2] * vel, u[3] * vel, (u[4] + press) * vel]
    parts[1 + d] = parts[1 + d] + press
    return parts, vel


def face_terms(low, up, d):
    inv_l, _, press_l, sound_l = primitives(low)
    inv_u, _, press_u, sound_u = primitives(up)
    flux_l, vel_l = flux_of(low, d, inv_l, press_l)
    flux_u, vel_u = flux_of(up, d, inv_u, press_u)
    lam = jnp.maximum(jnp.abs(vel_l) + sound_l, jnp.abs(vel_u) + sound_u)
    first, last = [], []
    for v in range(NV):
        central = HALF * (flux_u[v] - flux_l[v])
        jump = (HALF * lam) * (up[v] - low[v])
        first.append(-central - jump)
        last.append(jump - central)
    return first, last


def kernel(
    dims, sizes,
    state_hbm, reg_hbm, ly_hbm, wz_hbm, out_hbm, reg_out_hbm,
    out_ref, reg_out_ref, save_sem,
    state_ref, reg_ref, ly_ref, wz_ref, load_sem, u1_ref, acc_ref, fx_ref, fy_ref, fz_ref, sy_ref, sz_ref, step_ref,
    xh_ref, yp_ref, yh_ref, zp_ref, zh_ref, mcur_ref, mx_ref,
    xs_sem, xr_sem, ys_sem, yr_sem, zs_sem, zr_sem, ms_sem, mr_sem,
):
    nx, ny, nz = dims
    rows = nx * ny
    tiles = ny // SUB
    me = [lax.axis_index(a) for a in AXES]

    def peer(axis, offset):
        n = sizes[axis]
        return {AXES[axis]: lax.rem(me[axis] + (offset % n), n)}

    loads = [
        pltpu.make_async_copy(src, dst, load_sem.at[i])
        for i, (src, dst) in enumerate(
            ((state_hbm, state_ref), (ly_hbm, ly_ref), (wz_hbm, wz_ref), (reg_hbm, reg_ref))
        )
    ]
    for load in loads:
        load.start()

    barrier = pltpu.get_barrier_semaphore()
    greeted = 0
    for axis in range(3):
        for off in range(1, sizes[axis]):
            pl.semaphore_signal(barrier, inc=1, device_id=peer(axis, off), device_id_type=MESH)
            greeted += 1

    def remote(src, dst, ssem, rsem, axis, off):
        return pltpu.make_async_remote_copy(
            src_ref=src, dst_ref=dst, send_sem=ssem, recv_sem=rsem,
            device_id=peer(axis, off), device_id_type=MESH,
        )

    def x_copy(u_ref, sec, side, t):
        base = (rows - ny if side == 0 else 0) + t * SUB
        return remote(
            u_ref.at[:, pl.ds(base, SUB), :], xh_ref.at[sec, side, :, pl.ds(t * SUB, SUB), :],
            xs_sem.at[sec, side, t], xr_sem.at[sec, side, t], 0, 1 if side == 0 else -1,
        )

    def y_copy(sec, side):
        return remote(
            yp_ref.at[sec, 1 - side], yh_ref.at[sec, side],
            ys_sem.at[sec, side], yr_sem.at[sec, side], 1, 1 if side == 0 else -1,
        )

    def z_copy(sec, side):
        return remote(
            zp_ref.at[sec, 1 - side], zh_ref.at[sec, side],
            zs_sem.at[sec, side], zr_sem.at[sec, side], 2, 1 if side == 0 else -1,
        )

    def m_copy(axis, off):
        return remote(
            mcur_ref.at[axis], mx_ref.at[axis, off],
            ms_sem.at[axis, off], mr_sem.at[axis, off], axis, off,
        )

    lane_ids = lax.broadcasted_iota(jnp.int32, (ny, LANE), 1)

    def pack(u_ref, sec):
        for v in range(NV):
            for x in range(nx):
                a = x * ny
                yp_ref[sec, 0, v, x : x + 1, :] = u_ref[v, a : a + 1, :]
                yp_ref[sec, 1, v, x : x + 1, :] = u_ref[v, a + ny - 1 : a + ny, :]

        def one(v, carry):
            first = jnp.ones((ny, LANE), jnp.float32)
            last = first
            for x in range(nx):
                r = slice(x * ny, x * ny + ny)
                first = jnp.where(lane_ids == x, u_ref[v, r, 0:LANE][:, 0:1], first)
                last = jnp.where(lane_ids == x, u_ref[v, r, nz - LANE : nz][:, LANE - 1 : LANE], last)
            zp_ref[sec, 0, v] = first
            zp_ref[sec, 1, v] = last
            return carry

        lax.fori_loop(0, NV, one, 0)

    def pointwise(u_ref, lo, hi):
        def one(t, carry):
            r = pl.ds(pl.multiple_of(t * SUB, SUB), SUB)
            u = [u_ref[v, r, :] for v in range(NV)]
            inv, _, press, sound = primitives(u)
            for d, f_ref in enumerate((fx_ref, fy_ref, fz_ref)):
                parts, vel = flux_of(u, d, inv, press)
                for v in range(NV):
                    f_ref[v, r, :] = parts[v]
                if d == 1:
                    sy_ref[r, :] = jnp.abs(vel) + sound
                if d == 2:
                    sz_ref[r, :] = jnp.abs(vel) + sound
            return carry

        lax.fori_loop(lo, hi, one, 0)

    def local_max():
        def one(t, top):
            r = pl.ds(pl.multiple_of(t * SUB, SUB), SUB)
            u = [state_ref[v, r, :] for v in range(NV)]
            inv, mom_sq, _, sound = primitives(u)
            speed = jnp.sqrt(mom_sq) * inv + sound
            for b in range(nz // LANE):
                top = jnp.maximum(top, speed[:, b * LANE : (b + 1) * LANE])
            return top

        return lax.fori_loop(0, nx * tiles, one, jnp.zeros((SUB, LANE), jnp.float32))

    def halves(x):
        high = x.astype(jnp.bfloat16)
        return high, (x - high.astype(jnp.float32)).astype(jnp.bfloat16)

    def dot(a, b):
        return jnp.dot(a, b, preferred_element_type=jnp.float32)

    def products(v, carry):
        high, low = halves(fy_ref[v])
        acc_ref[v] = dot(ly_ref[0], high) + dot(ly_ref[0], low) + dot(ly_ref[1], high)
        high, low = halves(fz_ref[v])
        for w in range(nz // LANE - 1):
            c = slice(w * LANE, (w + 2) * LANE)
            acc_ref[v, :, c] += (
                dot(high[:, c], wz_ref[0, w]) + dot(low[:, c], wz_ref[0, w]) + dot(high[:, c], wz_ref[1, w])
            )
        return carry

    op_x = operator(nx)

    def along_x(t, carry):
        v = lax.div(t, tiles)
        base = lax.rem(t, tiles) * SUB
        where = [pl.ds(pl.multiple_of(base + i * ny, SUB), SUB) for i in range(nx)]
        f = [fx_ref[v, r, :] for r in where]
        for i in range(nx):
            total = acc_ref[v, where[i], :]
            for j in range(nx):
                if op_x[i, j] != 0.0:
                    total = total + float(op_x[i, j]) * f[j]
            acc_ref[v, where[i], :] = total
        return carry

    row_in = lax.broadcasted_iota(jnp.int32, (ny, nz), 0)
    lane_in = lax.broadcasted_iota(jnp.int32, (ny, nz), 1)

    def dissipate(u_ref):
        def one(x, carry):
            r = pl.ds(pl.multiple_of(x * ny, SUB), ny)
            s = sy_ref[r, :]
            mask = (lax.rem(row_in, NODES) == 0) & (row_in > 0)
            lam_y = jnp.where(mask, HALF * jnp.maximum(s, pltpu.roll(s, 1, 0)), 0.0)
            s = sz_ref[r, :]
            mask = (lax.rem(lane_in, NODES) == 0) & (lane_in > 0)
            lam_z = jnp.where(mask, HALF * jnp.maximum(s, pltpu.roll(s, 1, 1)), 0.0)
            for v in range(NV):
                u = u_ref[v, r, :]
                wy = lam_y * (u - pltpu.roll(u, 1, 0))
                wz = lam_z * (u - pltpu.roll(u, 1, 1))
                acc_ref[v, r, :] += (pltpu.roll(wy, ny - 1, 0) - wy) + (pltpu.roll(wz, nz - 1, 1) - wz)
            return carry

        lax.fori_loop(0, nx, one, 0)
        for e in range(NODES, nx, NODES):
            lo, up = (e - 1) * ny, e * ny
            for t in range(tiles):
                ra = slice(lo + t * SUB, lo + t * SUB + SUB)
                rb = slice(up + t * SUB, up + t * SUB + SUB)
                a = [u_ref[v, ra, :] for v in range(NV)]
                b = [u_ref[v, rb, :] for v in range(NV)]
                ia, _, _, ca = primitives(a)
                ib, _, _, cb = primitives(b)
                lam = HALF * jnp.maximum(jnp.abs(a[1] * ia) + ca, jnp.abs(b[1] * ib) + cb)
                for v in range(NV):
                    jump = lam * (b[v] - a[v])
                    acc_ref[v, rb, :] -= jump
                    acc_ref[v, ra, :] += jump

    def volume(u_ref):
        lax.fori_loop(0, NV, products, 0)
        lax.fori_loop(0, NV * tiles, along_x, 0)
        dissipate(u_ref)

    def edges_y(sec):
        for side in range(2):
            y_copy(sec, side).wait_recv()
            own = [yp_ref[sec, side, v] for v in range(NV)]
            other = [yh_ref[sec, side, v] for v in range(NV)]
            corr = face_terms(other, own, 1)[0] if side == 0 else face_terms(own, other, 1)[1]
            for v in range(NV):
                for x in range(nx):
                    a = x * ny + (0 if side == 0 else ny - 1)
                    acc_ref[v, a : a + 1, :] += corr[v][x : x + 1, :]

    def edges_z(sec):
        for side in range(2):
            z_copy(sec, side).wait_recv()
            own = [zp_ref[sec, side, v] for v in range(NV)]
            other = [zh_ref[sec, side, v] for v in range(NV)]
            corr = face_terms(other, own, 2)[0] if side == 0 else face_terms(own, other, 2)[1]
            at = 0 if side == 0 else LANE - 1
            c = slice(0, LANE) if side == 0 else slice(nz - LANE, nz)
            for v in range(NV):
                for x in range(nx):
                    r = slice(x * ny, x * ny + ny)
                    acc_ref[v, r, c] += jnp.where(lane_ids == at, corr[v][:, x : x + 1], 0.0)

    def advance(sec, r, corr=None):
        coef_a, coef_b = COEFFS[sec]
        src, old = (state_ref, reg_ref) if sec == 0 else (u1_ref, reg_out_ref)
        dst = u1_ref if sec == 0 else out_ref
        step = step_ref[...]
        for v in range(NV):
            res = acc_ref[v, r, :]
            if corr is not None:
                res = res + corr[v]
            k = coef_a * old[v, r, :] + step * res
            reg_out_ref[v, r, :] = k
            dst[v, r, :] = src[v, r, :] + coef_b * k

    def advance_inner(sec):
        def one(t, carry):
            advance(sec, pl.ds(pl.multiple_of(t * SUB, SUB), SUB))
            return carry

        lax.fori_loop(tiles, (nx - 1) * tiles, one, 0)

    def advance_outer(u_ref, sec, side, t):
        x_copy(u_ref, sec, side, t).wait_recv()
        base = (0 if side == 0 else rows - ny) + t * SUB
        r = slice(base, base + SUB)
        own = [u_ref[v, r, :] for v in range(NV)]
        other = [xh_ref[sec, side, v, t * SUB : (t + 1) * SUB, :] for v in range(NV)]
        corr = face_terms(other, own, 0)[0] if side == 0 else face_terms(own, other, 0)[1]
        advance(sec, r, corr)

    def reduce_max(axis, top):
        for off in range(1, sizes[axis]):
            m_copy(axis, off).wait_recv()
            top = jnp.maximum(top, mx_ref[axis, off])
        return top

    def send_max(axis):
        for off in range(1, sizes[axis]):
            m_copy(axis, off).start()

    order = [(t, side) for t in range(tiles) for side in range(2)]
    loads[0].wait()
    top = local_max()
    mcur_ref[0] = top
    pack(state_ref, 0)
    pl.semaphore_wait(barrier, greeted)
    send_max(0)
    for t, side in order:
        x_copy(state_ref, 0, side, t).start()
    pointwise(state_ref, 0, nx * tiles)
    top = reduce_max(0, top)
    mcur_ref[1] = top
    loads[1].wait()
    loads[2].wait()
    send_max(1)
    lax.fori_loop(0, NV, products, 0)
    top = reduce_max(1, top)
    mcur_ref[2] = top
    loads[3].wait()
    send_max(2)
    for side in range(2):
        y_copy(0, side).start()
        z_copy(0, side).start()
    lax.fori_loop(0, NV * tiles, along_x, 0)
    dissipate(state_ref)
    top = reduce_max(2, top)
    top = jnp.max(jnp.max(top, axis=0, keepdims=True), axis=1, keepdims=True)
    step_ref[...] = jnp.broadcast_to(COURANT * ELEM_WIDTH / (11.0 * top), (SUB, nz))
    edges_y(0)
    edges_z(0)
    advance_inner(0)
    pointwise(u1_ref, tiles, (nx - 1) * tiles)
    for t, side in order:
        advance_outer(state_ref, 0, side, t)
        x_copy(u1_ref, 1, 1 - side, t).start()
    pack(u1_ref, 1)
    pointwise(u1_ref, 0, tiles)
    for side in range(2):
        y_copy(1, side).start()
        z_copy(1, side).start()
    pointwise(u1_ref, (nx - 1) * tiles, nx * tiles)
    volume(u1_ref)
    edges_y(1)
    edges_z(1)
    advance_inner(1)
    saves = []

    def save(lo, size):
        for src, dst in ((out_ref, out_hbm), (reg_out_ref, reg_out_hbm)):
            r = pl.ds(lo, size)
            saves.append(pltpu.make_async_copy(src.at[:, r, :], dst.at[:, r, :], save_sem.at[len(saves)]))
            saves[-1].start()

    if nx > 2:
        save(ny, rows - 2 * ny)
    for t, side in order:
        advance_outer(u1_ref, 1, 1 - side, t)
        save((rows - ny if side == 0 else 0) + t * SUB, SUB)
    for axis in range(3):
        for off in range(1, sizes[axis]):
            m_copy(axis, off).wait_send()
    for sec in range(2):
        for side in range(2):
            y_copy(sec, side).wait_send()
            z_copy(sec, side).wait_send()
            for t in range(tiles):
                x_copy(state_ref if sec == 0 else u1_ref, sec, side, t).wait_send()
    for copy in saves:
        copy.wait()


def shards(sizes, state, register):
    nx, ny, nz = state.shape[1:]
    rows = nx * ny
    tiles = ny // SUB
    most = max(sizes)
    f32 = jnp.float32
    flat = (NV, rows, nz)
    ly = jnp.asarray(split(np.kron(np.eye(nx), operator(ny))))
    wz = jnp.asarray(split(windows(nz)))
    dma = pltpu.SemaphoreType.DMA
    new_state, new_reg = pl.pallas_call(
        functools.partial(kernel, (nx, ny, nz), sizes),
        out_shape=[jax.ShapeDtypeStruct(flat, f32)] * 2,
        in_specs=[pl.BlockSpec(memory_space=pltpu.HBM)] * 4,
        out_specs=[pl.BlockSpec(memory_space=pl.ANY)] * 2,
        scratch_shapes=[
            pltpu.VMEM(flat, f32), pltpu.VMEM(flat, f32), dma((2 + 4 * tiles,)),
            pltpu.VMEM(flat, f32), pltpu.VMEM(flat, f32),
            pltpu.VMEM(ly.shape, ly.dtype), pltpu.VMEM(wz.shape, wz.dtype), dma((4,)),
            pltpu.VMEM(flat, f32), pltpu.VMEM(flat, f32),
            pltpu.VMEM(flat, f32), pltpu.VMEM(flat, f32), pltpu.VMEM(flat, f32),
            pltpu.VMEM((rows, nz), f32), pltpu.VMEM((rows, nz), f32),
            pltpu.VMEM((SUB, nz), f32),
            pltpu.VMEM((2, 2, NV, ny, nz), f32),
            pltpu.VMEM((2, 2, NV, nx, nz), f32), pltpu.VMEM((2, 2, NV, nx, nz), f32),
            pltpu.VMEM((2, 2, NV, ny, LANE), f32), pltpu.VMEM((2, 2, NV, ny, LANE), f32),
            pltpu.VMEM((3, SUB, LANE), f32), pltpu.VMEM((3, most, SUB, LANE), f32),
            dma((2, 2, tiles)), dma((2, 2, tiles)), dma((2, 2)), dma((2, 2)),
            dma((2, 2)), dma((2, 2)), dma((3, most)), dma((3, most)),
        ],
        compiler_params=pltpu.CompilerParams(
            collective_id=0, has_side_effects=True, vmem_limit_bytes=GRANT
        ),
        name="dg_step",
    )(state.reshape(flat), register.reshape(flat), ly, wz)
    return new_state.reshape(state.shape), new_reg.reshape(state.shape)


def solution(mesh):
    sizes = tuple(mesh.shape[a] for a in AXES)
    spec = P(None, "gx", "gy", "gz")
    return jax.shard_map(
        functools.partial(shards, sizes),
        mesh=mesh,
        in_specs=(spec, spec),
        out_specs=(spec, spec),
        check_vma=False,
    )
```

```python
import functools
import math

import jax
import jax.numpy as jnp
import numpy as np
from jax import lax
from jax.experimental import pallas as pl
from jax.experimental.pallas import tpu as pltpu
from jax.sharding import PartitionSpec as P

GAMMA = 1.4
GM1 = 0.4
ELEM_WIDTH = 0.05
COURANT = 0.5
INV_W = 15.0
SCALE = 2.0 / ELEM_WIDTH
HALF = 0.5 * INV_W * SCALE
COEFFS = (
    (-567301805773.0 / 1357537059087.0, 5161836677717.0 / 13612068292357.0),
    (-2404267990393.0 / 2016746695238.0, 1720146321549.0 / 2090206949498.0),
)
AXES = ("gx", "gy", "gz")
NV = 5
SUB = 8
LANE = 128
GRANT = 60 * 1024 * 1024
MESH = pl.DeviceIdType.MESH


def gll_derivative():
    seven = math.sqrt(7.0)
    inner = math.sqrt(1.0 / 3.0 - 2.0 * seven / 21.0)
    outer = math.sqrt(1.0 / 3.0 + 2.0 * seven / 21.0)
    points = np.array([-1.0, -outer, -inner, inner, outer, 1.0])
    count = len(points)
    weights = np.array(
        [np.prod([points[i] - points[j] for j in range(count) if j != i]) for i in range(count)]
    )
    table = np.zeros((count, count))
    for i in range(count):
        for j in range(count):
            if i != j:
                table[i, j] = weights[i] / weights[j] / (points[i] - points[j])
        table[i, i] = -np.sum(table[i])
    return table


DMAT = gll_derivative()
NODES = DMAT.shape[0]


def operator(length):
    op = np.kron(np.eye(length // NODES), -SCALE * DMAT)
    for j in range(NODES, length, NODES):
        i = j - 1
        op[j, j] -= HALF
        op[j, i] += HALF
        op[i, j] -= HALF
        op[i, i] += HALF
    op[np.abs(op) < 1e-9] = 0.0
    return op


def split(table):
    high = np.asarray(table, np.float32).astype(jnp.bfloat16)
    low = (np.asarray(table, np.float32) - high.astype(np.float32)).astype(jnp.bfloat16)
    return np.stack([high, low])


def windows(length):
    op = operator(length).T
    count = length // LANE - 1
    out = np.zeros((count, 2 * LANE, 2 * LANE))
    for w in range(count):
        lo = 0 if w == 0 else LANE // 2
        hi = 2 * LANE if w == count - 1 else LANE + LANE // 2
        base = w * LANE
        out[w, :, lo:hi] = op[base : base + 2 * LANE, base + lo : base + hi]
    return out


def primitives(u):
    inv = 1.0 / u[0]
    mom_sq = u[1] * u[1] + u[2] * u[2] + u[3] * u[3]
    press = GM1 * (u[4] - 0.5 * mom_sq * inv)
    sound = jnp.sqrt(GAMMA * press * inv)
    return inv, mom_sq, press, sound


def flux_of(u, d, inv, press):
    vel = u[1 + d] * inv
    parts = [u[1 + d], u[1] * vel, u[2] * vel, u[3] * vel, (u[4] + press) * vel]
    parts[1 + d] = parts[1 + d] + press
    return parts, vel


def face_terms(low, up, d):
    inv_l, _, press_l, sound_l = primitives(low)
    inv_u, _, press_u, sound_u = primitives(up)
    flux_l, vel_l = flux_of(low, d, inv_l, press_l)
    flux_u, vel_u = flux_of(up, d, inv_u, press_u)
    lam = jnp.maximum(jnp.abs(vel_l) + sound_l, jnp.abs(vel_u) + sound_u)
    first, last = [], []
    for v in range(NV):
        central = HALF * (flux_u[v] - flux_l[v])
        jump = (HALF * lam) * (up[v] - low[v])
        first.append(-central - jump)
        last.append(jump - central)
    return first, last


def kernel(
    dims, sizes,
    state_hbm, reg_hbm, ly_hbm, wz_hbm, out_hbm, reg_out_hbm,
    out_ref, reg_out_ref, save_sem,
    state_ref, reg_ref, ly_ref, wz_ref, load_sem, u1_ref, acc_ref, fx_ref, fy_ref, fz_ref, sy_ref, sz_ref, step_ref,
    xh_ref, yp_ref, yh_ref, zp_ref, zh_ref, mcur_ref, mx_ref,
    xs_sem, xr_sem, ys_sem, yr_sem, zs_sem, zr_sem, ms_sem, mr_sem,
):
    nx, ny, nz = dims
    rows = nx * ny
    tiles = ny // SUB
    me = [lax.axis_index(a) for a in AXES]

    def peer(axis, offset):
        n = sizes[axis]
        return {AXES[axis]: lax.rem(me[axis] + (offset % n), n)}

    loads = [
        pltpu.make_async_copy(src, dst, load_sem.at[i])
        for i, (src, dst) in enumerate(
            ((state_hbm, state_ref), (ly_hbm, ly_ref), (wz_hbm, wz_ref), (reg_hbm, reg_ref))
        )
    ]
    for load in loads:
        load.start()

    barrier = pltpu.get_barrier_semaphore()
    greeted = 0
    for axis in range(3):
        for off in range(1, sizes[axis]):
            pl.semaphore_signal(barrier, inc=1, device_id=peer(axis, off), device_id_type=MESH)
            greeted += 1

    def remote(src, dst, ssem, rsem, axis, off):
        return pltpu.make_async_remote_copy(
            src_ref=src, dst_ref=dst, send_sem=ssem, recv_sem=rsem,
            device_id=peer(axis, off), device_id_type=MESH,
        )

    def x_copy(u_ref, sec, side, t):
        base = (rows - ny if side == 0 else 0) + t * SUB
        return remote(
            u_ref.at[:, pl.ds(base, SUB), :], xh_ref.at[sec, side, :, pl.ds(t * SUB, SUB), :],
            xs_sem.at[sec, side, t], xr_sem.at[sec, side, t], 0, 1 if side == 0 else -1,
        )

    def y_copy(sec, side):
        return remote(
            yp_ref.at[sec, 1 - side], yh_ref.at[sec, side],
            ys_sem.at[sec, side], yr_sem.at[sec, side], 1, 1 if side == 0 else -1,
        )

    def z_copy(sec, side):
        return remote(
            zp_ref.at[sec, 1 - side], zh_ref.at[sec, side],
            zs_sem.at[sec, side], zr_sem.at[sec, side], 2, 1 if side == 0 else -1,
        )

    def m_copy(axis, off):
        return remote(
            mcur_ref.at[axis], mx_ref.at[axis, off],
            ms_sem.at[axis, off], mr_sem.at[axis, off], axis, off,
        )

    lane_ids = lax.broadcasted_iota(jnp.int32, (ny, LANE), 1)

    def pack(u_ref, sec):
        for v in range(NV):
            for x in range(nx):
                a = x * ny
                yp_ref[sec, 0, v, x : x + 1, :] = u_ref[v, a : a + 1, :]
                yp_ref[sec, 1, v, x : x + 1, :] = u_ref[v, a + ny - 1 : a + ny, :]

        def one(v, carry):
            first = jnp.ones((ny, LANE), jnp.float32)
            last = first
            for x in range(nx):
                r = slice(x * ny, x * ny + ny)
                first = jnp.where(lane_ids == x, u_ref[v, r, 0:LANE][:, 0:1], first)
                last = jnp.where(lane_ids == x, u_ref[v, r, nz - LANE : nz][:, LANE - 1 : LANE], last)
            zp_ref[sec, 0, v] = first
            zp_ref[sec, 1, v] = last
            return carry

        lax.fori_loop(0, NV, one, 0)

    def pointwise(u_ref, lo, hi):
        def one(t, carry):
            r = pl.ds(pl.multiple_of(t * SUB, SUB), SUB)
            u = [u_ref[v, r, :] for v in range(NV)]
            inv, _, press, sound = primitives(u)
            for d, f_ref in enumerate((fx_ref, fy_ref, fz_ref)):
                parts, vel = flux_of(u, d, inv, press)
                for v in range(NV):
                    f_ref[v, r, :] = parts[v]
                if d == 1:
                    sy_ref[r, :] = jnp.abs(vel) + sound
                if d == 2:
                    sz_ref[r, :] = jnp.abs(vel) + sound
            return carry

        lax.fori_loop(lo, hi, one, 0)

    def local_max():
        def one(t, top):
            r = pl.ds(pl.multiple_of(t * SUB, SUB), SUB)
            u = [state_ref[v, r, :] for v in range(NV)]
            inv, mom_sq, _, sound = primitives(u)
            speed = jnp.sqrt(mom_sq) * inv + sound
            for b in range(nz // LANE):
                top = jnp.maximum(top, speed[:, b * LANE : (b + 1) * LANE])
            return top

        return lax.fori_loop(0, nx * tiles, one, jnp.zeros((SUB, LANE), jnp.float32))

    def halves(x):
        high = x.astype(jnp.bfloat16)
        return high, (x - high.astype(jnp.float32)).astype(jnp.bfloat16)

    def dot(a, b):
        return jnp.dot(a, b, preferred_element_type=jnp.float32)

    def products(v, carry):
        high, low = halves(fy_ref[v])
        acc_ref[v] = dot(ly_ref[0], high) + dot(ly_ref[0], low) + dot(ly_ref[1], high)
        high, low = halves(fz_ref[v])
        for w in range(nz // LANE - 1):
            c = slice(w * LANE, (w + 2) * LANE)
            acc_ref[v, :, c] += (
                dot(high[:, c], wz_ref[0, w]) + dot(low[:, c], wz_ref[0, w]) + dot(high[:, c], wz_ref[1, w])
            )
        return carry

    op_x = operator(nx)

    def along_x(t, carry):
        v = lax.div(t, tiles)
        base = lax.rem(t, tiles) * SUB
        where = [pl.ds(pl.multiple_of(base + i * ny, SUB), SUB) for i in range(nx)]
        f = [fx_ref[v, r, :] for r in where]
        for i in range(nx):
            total = acc_ref[v, where[i], :]
            for j in range(nx):
                if op_x[i, j] != 0.0:
                    total = total + float(op_x[i, j]) * f[j]
            acc_ref[v, where[i], :] = total
        return carry

    row_in = lax.broadcasted_iota(jnp.int32, (ny, nz), 0)
    lane_in = lax.broadcasted_iota(jnp.int32, (ny, nz), 1)

    def dissipate(u_ref):
        def one(x, carry):
            r = pl.ds(pl.multiple_of(x * ny, SUB), ny)
            s = sy_ref[r, :]
            mask = (lax.rem(row_in, NODES) == 0) & (row_in > 0)
            lam_y = jnp.where(mask, HALF * jnp.maximum(s, pltpu.roll(s, 1, 0)), 0.0)
            s = sz_ref[r, :]
            mask = (lax.rem(lane_in, NODES) == 0) & (lane_in > 0)
            lam_z = jnp.where(mask, HALF * jnp.maximum(s, pltpu.roll(s, 1, 1)), 0.0)
            for v in range(NV):
                u = u_ref[v, r, :]
                wy = lam_y * (u - pltpu.roll(u, 1, 0))
                wz = lam_z * (u - pltpu.roll(u, 1, 1))
                acc_ref[v, r, :] += (pltpu.roll(wy, ny - 1, 0) - wy) + (pltpu.roll(wz, nz - 1, 1) - wz)
            return carry

        lax.fori_loop(0, nx, one, 0)
        for e in range(NODES, nx, NODES):
            lo, up = (e - 1) * ny, e * ny
            for t in range(tiles):
                ra = slice(lo + t * SUB, lo + t * SUB + SUB)
                rb = slice(up + t * SUB, up + t * SUB + SUB)
                a = [u_ref[v, ra, :] for v in range(NV)]
                b = [u_ref[v, rb, :] for v in range(NV)]
                ia, _, _, ca = primitives(a)
                ib, _, _, cb = primitives(b)
                lam = HALF * jnp.maximum(jnp.abs(a[1] * ia) + ca, jnp.abs(b[1] * ib) + cb)
                for v in range(NV):
                    jump = lam * (b[v] - a[v])
                    acc_ref[v, rb, :] -= jump
                    acc_ref[v, ra, :] += jump

    def volume(u_ref):
        lax.fori_loop(0, NV, products, 0)
        lax.fori_loop(0, NV * tiles, along_x, 0)
        dissipate(u_ref)

    def edges_y(sec):
        for side in range(2):
            y_copy(sec, side).wait_recv()
            own = [yp_ref[sec, side, v] for v in range(NV)]
            other = [yh_ref[sec, side, v] for v in range(NV)]
            corr = face_terms(other, own, 1)[0] if side == 0 else face_terms(own, other, 1)[1]
            for v in range(NV):
                for x in range(nx):
                    a = x * ny + (0 if side == 0 else ny - 1)
                    acc_ref[v, a : a + 1, :] += corr[v][x : x + 1, :]

    def edges_z(sec):
        for side in range(2):
            z_copy(sec, side).wait_recv()
            own = [zp_ref[sec, side, v] for v in range(NV)]
            other = [zh_ref[sec, side, v] for v in range(NV)]
            corr = face_terms(other, own, 2)[0] if side == 0 else face_terms(own, other, 2)[1]
            at = 0 if side == 0 else LANE - 1
            c = slice(0, LANE) if side == 0 else slice(nz - LANE, nz)
            for v in range(NV):
                for x in range(nx):
                    r = slice(x * ny, x * ny + ny)
                    acc_ref[v, r, c] += jnp.where(lane_ids == at, corr[v][:, x : x + 1], 0.0)

    def advance(sec, r, corr=None):
        coef_a, coef_b = COEFFS[sec]
        src, old = (state_ref, reg_ref) if sec == 0 else (u1_ref, reg_out_ref)
        dst = u1_ref if sec == 0 else out_ref
        step = step_ref[...]
        for v in range(NV):
            res = acc_ref[v, r, :]
            if corr is not None:
                res = res + corr[v]
            k = coef_a * old[v, r, :] + step * res
            reg_out_ref[v, r, :] = k
            dst[v, r, :] = src[v, r, :] + coef_b * k

    def advance_inner(sec):
        def one(t, carry):
            advance(sec, pl.ds(pl.multiple_of(t * SUB, SUB), SUB))
            return carry

        lax.fori_loop(tiles, (nx - 1) * tiles, one, 0)

    def advance_outer(u_ref, sec, side, t):
        x_copy(u_ref, sec, side, t).wait_recv()
        base = (0 if side == 0 else rows - ny) + t * SUB
        r = slice(base, base + SUB)
        own = [u_ref[v, r, :] for v in range(NV)]
        other = [xh_ref[sec, side, v, t * SUB : (t + 1) * SUB, :] for v in range(NV)]
        corr = face_terms(other, own, 0)[0] if side == 0 else face_terms(own, other, 0)[1]
        advance(sec, r, corr)

    def reduce_max(axis, top):
        for off in range(1, sizes[axis]):
            m_copy(axis, off).wait_recv()
            top = jnp.maximum(top, mx_ref[axis, off])
        return top

    def send_max(axis):
        for off in range(1, sizes[axis]):
            m_copy(axis, off).start()

    order = [(t, side) for t in range(tiles) for side in range(2)]
    pl.semaphore_wait(barrier, greeted)
    for t, side in order[:2]:
        x_copy(state_hbm, 0, side, t).start()
    loads[0].wait()
    top = local_max()
    mcur_ref[0] = top
    pack(state_ref, 0)
    send_max(0)
    for t, side in order[2:]:
        x_copy(state_hbm, 0, side, t).start()
    pointwise(state_ref, 0, nx * tiles)
    top = reduce_max(0, top)
    mcur_ref[1] = top
    loads[1].wait()
    loads[2].wait()
    send_max(1)
    lax.fori_loop(0, NV, products, 0)
    top = reduce_max(1, top)
    mcur_ref[2] = top
    loads[3].wait()
    send_max(2)
    for side in range(2):
        y_copy(0, side).start()
        z_copy(0, side).start()
    lax.fori_loop(0, NV * tiles, along_x, 0)
    dissipate(state_ref)
    edges_y(0)
    edges_z(0)
    top = reduce_max(2, top)
    top = jnp.max(jnp.max(top, axis=0, keepdims=True), axis=1, keepdims=True)
    step_ref[...] = jnp.broadcast_to(COURANT * ELEM_WIDTH / (11.0 * top), (SUB, nz))
    advance_inner(0)
    pointwise(u1_ref, tiles, (nx - 1) * tiles)
    for t, side in order:
        advance_outer(state_ref, 0, side, t)
        x_copy(u1_ref, 1, 1 - side, t).start()
    pack(u1_ref, 1)
    pointwise(u1_ref, 0, tiles)
    for side in range(2):
        y_copy(1, side).start()
        z_copy(1, side).start()
    pointwise(u1_ref, (nx - 1) * tiles, nx * tiles)
    volume(u1_ref)
    edges_y(1)
    edges_z(1)
    advance_inner(1)
    saves = []

    def save(lo, size):
        for src, dst in ((out_ref, out_hbm), (reg_out_ref, reg_out_hbm)):
            r = pl.ds(lo, size)
            saves.append(pltpu.make_async_copy(src.at[:, r, :], dst.at[:, r, :], save_sem.at[len(saves)]))
            saves[-1].start()

    if nx > 2:
        save(ny, rows - 2 * ny)
    for t, side in order:
        advance_outer(u1_ref, 1, 1 - side, t)
        save((rows - ny if side == 0 else 0) + t * SUB, SUB)
    for axis in range(3):
        for off in range(1, sizes[axis]):
            m_copy(axis, off).wait_send()
    for sec in range(2):
        for side in range(2):
            y_copy(sec, side).wait_send()
            z_copy(sec, side).wait_send()
            for t in range(tiles):
                x_copy(state_hbm if sec == 0 else u1_ref, sec, side, t).wait_send()
    for copy in saves:
        copy.wait()


def shards(sizes, state, register):
    nx, ny, nz = state.shape[1:]
    rows = nx * ny
    tiles = ny // SUB
    most = max(sizes)
    f32 = jnp.float32
    flat = (NV, rows, nz)
    ly = jnp.asarray(split(np.kron(np.eye(nx), operator(ny))))
    wz = jnp.asarray(split(windows(nz)))
    dma = pltpu.SemaphoreType.DMA
    new_state, new_reg = pl.pallas_call(
        functools.partial(kernel, (nx, ny, nz), sizes),
        out_shape=[jax.ShapeDtypeStruct(flat, f32)] * 2,
        in_specs=[pl.BlockSpec(memory_space=pltpu.HBM)] * 4,
        out_specs=[pl.BlockSpec(memory_space=pl.ANY)] * 2,
        scratch_shapes=[
            pltpu.VMEM(flat, f32), pltpu.VMEM(flat, f32), dma((2 + 4 * tiles,)),
            pltpu.VMEM(flat, f32), pltpu.VMEM(flat, f32),
            pltpu.VMEM(ly.shape, ly.dtype), pltpu.VMEM(wz.shape, wz.dtype), dma((4,)),
            pltpu.VMEM(flat, f32), pltpu.VMEM(flat, f32),
            pltpu.VMEM(flat, f32), pltpu.VMEM(flat, f32), pltpu.VMEM(flat, f32),
            pltpu.VMEM((rows, nz), f32), pltpu.VMEM((rows, nz), f32),
            pltpu.VMEM((SUB, nz), f32),
            pltpu.VMEM((2, 2, NV, ny, nz), f32),
            pltpu.VMEM((2, 2, NV, nx, nz), f32), pltpu.VMEM((2, 2, NV, nx, nz), f32),
            pltpu.VMEM((2, 2, NV, ny, LANE), f32), pltpu.VMEM((2, 2, NV, ny, LANE), f32),
            pltpu.VMEM((3, SUB, LANE), f32), pltpu.VMEM((3, most, SUB, LANE), f32),
            dma((2, 2, tiles)), dma((2, 2, tiles)), dma((2, 2)), dma((2, 2)),
            dma((2, 2)), dma((2, 2)), dma((3, most)), dma((3, most)),
        ],
        compiler_params=pltpu.CompilerParams(
            collective_id=0, has_side_effects=True, vmem_limit_bytes=GRANT
        ),
        name="dg_step",
    )(state.reshape(flat), register.reshape(flat), ly, wz)
    return new_state.reshape(state.shape), new_reg.reshape(state.shape)


def solution(mesh):
    sizes = tuple(mesh.shape[a] for a in AXES)
    spec = P(None, "gx", "gy", "gz")
    return jax.shard_map(
        functools.partial(shards, sizes),
        mesh=mesh,
        in_specs=(spec, spec),
        out_specs=(spec, spec),
        check_vma=False,
    )
```
